128 devices in a mesh: phi: 8 (over y, z_hi), theta: 16 (over x, z_lo, core).
Axes of the slice: x: 4, y: 4, z: 4 (z_hi: 2, z_lo: 2; z = z_hi * 2 + z_lo), core: 2. Of those that a mesh axis runs over, the one named last changes fastest.
Arguments:
- subtree_pattern: bfloat16 [1024, 2, 32, 64, 128], P(('phi', 'theta')), may hold values from -6 to 6
- up_phi: bfloat16 [128, 256], replicated, may hold values from -0.5 to 0.5
- up_theta: bfloat16 [128, 64], replicated, may hold values from -0.75 to 0.75
- offsets: float32 [3, 1024], P(None, ('phi', 'theta')), may hold values from -8 to 8
- theta_start: int32 [512], P('theta'), may hold values from -2 to 126, as said below
- theta_frac: float32 [512], P('theta'), may hold values from 0 to 1
- phi_start: int32 [2048], P('phi'), may hold values from -2 to 254, as said below
- phi_frac: float32 [2048], P('phi'), may hold values from 0 to 1
Outputs:
- rcs: float32 [16, 512, 2048], P(None, 'theta', 'phi')
The draws below stay inside these ranges and needn't reach their ends.
Inputs may be any that keep to these rules, and one draw needn't show every extreme that they name: `theta_start`: row o lies in polar band b = o // 32; its start is b * (128 // 16) + k with k from -2 to 128 // 16 - 2; the first row of each band has k = -2 and the last k = 128 // 16 - 2. `phi_start`: column w lies in azimuth band b = w // 256; its start is b * (256 // 8) + k with k from -2 to 256 // 8 - 2, read periodically; the first column of each band has k = -2 and the last k = 256 // 8 - 2.
All inputs are finite; a program needn't handle non-finite values.
Results may differ from the reference program's by a relative error of at most 0.0024.
Values sent between devices are 32-bit elements; how exact they have to be, the bound alone decides.
No kernel may reach another device: no remote copies, remote signals or barrier semaphores. Data moves between devices by JAX's collectives and lax.ppermute only.
A program may use at most 128 MiB of HBM per device.

```python
import math
import jax
import jax.numpy as jnp
from jax import lax

NT = 128
NP = 256
MT = 64
MP = 128
INC = 16
OT_DEV = 32
OP_DEV = 256
QUANT = 32
SUBTREES = 1024
NOT = 512
NOP = 2048
N_PHI = 8
N_THETA = 16


def band_starts(key, total_rows, rows_band, nodes_band):
    rows = jnp.arange(total_rows, dtype=jnp.int32)
    band = rows // rows_band
    within = rows % rows_band
    drawn = jax.random.randint(jax.random.fold_in(key, 7), (total_rows,), -2, nodes_band - 1)
    drawn = jnp.where(within == 0, -2, jnp.where(within == rows_band - 1, nodes_band - 2, drawn))
    return (band * nodes_band + drawn).astype(jnp.int32)


def draw_theta_start(key, part):
    return band_starts(key, NOT, OT_DEV, NT // N_THETA)


def draw_phi_start(key, part):
    return band_starts(key, NOP, OP_DEV, NP // N_PHI)


def level_of(own_key, extent, pieces, smallest, top_value):
    factor_of = 1.0
    for axis_at, shards_of in pieces:
        heights = jax.random.uniform(jax.random.fold_in(jax.random.fold_in(own_key, 6), axis_at), (shards_of,), jnp.float32, smallest / len(pieces), top_value / len(pieces))
        factor_of = factor_of * jnp.repeat(jnp.exp(heights), extent[axis_at] // shards_of).reshape((-1,) + (1,) * (len(extent) - 1 - axis_at))
    return factor_of


def gaussian(stream_key, shape, deviation, most, split=(), kind=jnp.bfloat16):
    gain = level_of(stream_key, shape, split, -0.22, 0.18) if split else 1.0
    values = jax.random.normal(stream_key, shape, jnp.float32) * deviation * gain
    return jnp.minimum(jnp.maximum(values, -most), most).astype(kind)


def setup_inputs(seed: int = 0) -> dict:
    splits = jax.random.split(jax.random.key(seed), 9)
    subtree_pattern = gaussian(splits[0], (SUBTREES, 2, QUANT, MT, MP), 1.0, 6.0, ((0, 128),))
    up_phi = gaussian(splits[1], (MP, NP), MP ** -0.5, 0.5)
    up_theta = gaussian(splits[2], (NT, MT), MT ** -0.5, 0.75)
    offsets = jnp.clip(jax.random.uniform(splits[3], (3, SUBTREES), jnp.float32, -8.0, 8.0) * level_of(splits[3], (3, SUBTREES), ((1, 128),), -0.4, 0.0), -8.0, 8.0)
    theta_start = draw_theta_start(jax.random.fold_in(splits[8], 71), 0)
    theta_frac = jnp.clip(1.0 * jax.random.uniform(splits[5], (NOT,), jnp.float32) ** level_of(splits[5], (NOT,), ((0, 16),), -0.2, 0.2), 0.0, 1.0)
    phi_start = draw_phi_start(jax.random.fold_in(splits[8], 71), 0)
    phi_frac = jnp.clip(1.0 * jax.random.uniform(splits[7], (NOP,), jnp.float32) ** level_of(splits[7], (NOP,), ((0, 8),), -0.2, 0.2), 0.0, 1.0)
    return {"subtree_pattern": subtree_pattern, "up_phi": up_phi, "up_theta": up_theta, "offsets": offsets, "theta_start": theta_start, "theta_frac": theta_frac, "phi_start": phi_start, "phi_frac": phi_frac}


def directions():
    polar = (jnp.arange(NT, dtype=jnp.float32) + 0.5) * (math.pi / NT)
    azimuth = jnp.arange(NP, dtype=jnp.float32) * (2.0 * math.pi / NP)
    sine_polar = jnp.sin(polar)[:, None]
    unit_x = sine_polar * jnp.cos(azimuth)[None, :]
    unit_y = sine_polar * jnp.sin(azimuth)[None, :]
    unit_z = jnp.cos(polar)[:, None] * jnp.ones((1, NP), jnp.float32)
    return unit_x, unit_y, unit_z


def shift_centre(fine_grid, offset, unit_x, unit_y, unit_z):
    phase_angle = (2.0 * math.pi) * (offset[0] * unit_x + offset[1] * unit_y + offset[2] * unit_z)
    cosine = jnp.cos(phase_angle)
    sine_part = jnp.sin(phase_angle)
    real_part = fine_grid[0] * cosine - fine_grid[1] * sine_part
    imag_part = fine_grid[0] * sine_part + fine_grid[1] * cosine
    return jnp.stack([real_part, imag_part])


def lagrange_matrix(start, frac, width):
    position = 1.0 + frac
    weights = [-(position - 1.0) * (position - 2.0) * (position - 3.0) / 6.0,
               position * (position - 2.0) * (position - 3.0) / 2.0,
               -position * (position - 1.0) * (position - 3.0) / 2.0,
               position * (position - 1.0) * (position - 2.0) / 6.0]
    columns = jnp.arange(width, dtype=jnp.int32)[None, :]
    matrix = jnp.zeros((start.shape[0], width), frac.dtype)
    for tap in range(4):
        matrix = matrix + jnp.where(columns == (start + tap)[:, None], weights[tap][:, None], 0.0)
    return matrix


def reference(subtree_pattern, up_phi, up_theta, offsets, theta_start, theta_frac, phi_start, phi_frac):
    unit_x, unit_y, unit_z = directions()
    phi_matrix = up_phi.astype(jnp.float32)
    theta_matrix = up_theta.astype(jnp.float32)

    def add_subtree(total, inputs):
        pattern, offset = inputs
        coarse = jnp.einsum('rqmp,pn->rqmn', pattern.astype(jnp.float32), phi_matrix).astype(jnp.bfloat16)
        coarse = lax.optimization_barrier(coarse)
        fine_grid = jnp.einsum('tm,rqmn->rqtn', theta_matrix, coarse.astype(jnp.float32))
        return total + shift_centre(fine_grid, offset, unit_x, unit_y, unit_z), None

    zeros = jnp.zeros((2, QUANT, NT, NP), jnp.float32)
    root, ignored = lax.scan(add_subtree, zeros, (subtree_pattern, offsets.T))
    padded = jnp.pad(root, ((0, 0), (0, 0), (2, 2), (0, 0)))
    padded = jnp.concatenate([padded[..., NP - 2:], padded, padded[..., :2]], axis=3)
    theta_weights = lagrange_matrix(theta_start + 2, theta_frac, NT + 4)
    phi_weights = lagrange_matrix(phi_start + 2, phi_frac, NP + 4)
    field = jnp.einsum('ot,rqtp->rqop', theta_weights, padded, precision=lax.Precision.HIGHEST)
    field = jnp.einsum('rqop,wp->rqow', field, phi_weights, precision=lax.Precision.HIGHEST)
    power = (field * field).reshape(4, INC, NOT, NOP)
    return jnp.sum(power, axis=0) / SUBTREES
```

```python
import functools

import jax
import jax.numpy as jnp
from jax import lax
from jax.experimental import pallas as pl
from jax.experimental.pallas import tpu as pltpu
from jax.sharding import Mesh
from jax.sharding import PartitionSpec as P

NT = 128
NP = 256
F32 = jnp.float32
BF16 = jnp.bfloat16

CHUNKS = (("x", 0, 8), ("z", 16, 8), ("x", 8, 8), ("z", 24, 8))
AXES = {"x": "x", "z": ("zh", "zl"), "y": "y"}
THETA = ("x", "zl", "c")
PHI = ("y", "zh")

SIN = (6.283185005187988, -41.341590881347656, 81.59994506835938, -76.61446380615234,
       41.34282684326172, -12.47114372253418)
COS = (1.0, -19.73920440673828, 64.93911743164062, -85.45014190673828, 60.16762161254883,
       -25.96756935119629, 6.528613567352295)


def sincos_turns(turns):
    f = turns - jnp.round(turns)
    g = f * f
    s = jnp.full_like(g, SIN[-1])
    for coef in SIN[-2::-1]:
        s = s * g + coef
    c = jnp.full_like(g, COS[-1])
    for coef in COS[-2::-1]:
        c = c * g + coef
    return s * f, c


def iota(shape, dim):
    return lax.broadcasted_iota(jnp.int32, shape, dim)


def prep_kernel(core_ref, off_ref, uphi_ref, utheta_ref, table_ref, uphi_out, utheta_out):
    core = core_ref[0]
    row = iota((NT, NP), 0)
    theta = (row % 64) // 8 * 16 + ((row // 64) ^ core) * 8 + row % 8
    sin_t, cos_t = sincos_turns((theta.astype(F32) + 0.5) * (0.5 / NT))
    col = iota((NT, NP), 1)
    phi = (col % 128) // 32 * 64 + col // 128 * 32 + col % 32
    sin_p, cos_p = sincos_turns(phi.astype(F32) * (1.0 / NP))
    unit_x = sin_t * cos_p
    unit_y = sin_t * sin_p
    for s in range(table_ref.shape[0]):
        turns = off_ref[0, s] * unit_x + off_ref[1, s] * unit_y + off_ref[2, s] * cos_t
        sine, cosine = sincos_turns(turns)
        table_ref[s, 0] = cosine
        table_ref[s, 1] = sine
    src = iota((NP, NP), 0)
    dst = iota((NP, NP), 1)
    pick = ((dst % 128) // 32 * 64 + dst // 128 * 32 + dst % 32 == src).astype(F32).astype(BF16)
    uphi_out[...] = jnp.dot(uphi_ref[...], pick, preferred_element_type=F32).astype(BF16)
    r2 = iota((NT, NT), 0)
    th2 = (r2 % 64) // 8 * 16 + ((r2 // 64) ^ core) * 8 + r2 % 8
    pick2 = (iota((NT, NT), 1) == th2).astype(F32).astype(BF16)
    utheta_out[...] = jnp.dot(pick2, utheta_ref[...], preferred_element_type=F32).astype(BF16)


def main_kernel(uphi_ref, utheta_ref, table_ref, pat_ref, keep_ref, send_ref, *, order):
    subs = pat_ref.shape[0]
    coarse = []
    for s in range(subs):
        both = pat_ref[s, :, 0].reshape(128, 128)
        both = jnp.dot(both, uphi_ref[...], preferred_element_type=F32).astype(BF16)
        coarse.append(both.reshape(2, 64, NP))
    for half, out_ref in ((0, keep_ref), (1, send_ref)):
        rows = pl.ds(half * 64, 64)
        u = utheta_ref[rows, :]
        acc_r = jnp.zeros((64, NP), F32)
        acc_i = jnp.zeros((64, NP), F32)
        for s in range(subs):
            re = jnp.dot(u, coarse[s][0], preferred_element_type=F32)
            im = jnp.dot(u, coarse[s][1], preferred_element_type=F32)
            cosine = table_ref[s, 0, rows, :]
            sine = table_ref[s, 1, rows, :]
            acc_r = acc_r + (re * cosine - im * sine)
            acc_i = acc_i + (re * sine + im * cosine)
        for r, acc in ((0, acc_r), (1, acc_i)):
            for xi in range(4):
                for zl in range(2):
                    tile = acc[(xi * 2 + zl) * 8:(xi * 2 + zl) * 8 + 8]
                    for zh in range(2):
                        zi = zh * 2 + zl
                        at = (xi, zi) if order == "x" else (zi, xi)
                        out_ref[at[0], at[1], r, 0] = tile[:, zh * 128:zh * 128 + 128]


def main_call(order, first, count, uphi, utheta, table, pattern):
    subs = pattern.shape[0]
    out = jax.ShapeDtypeStruct((4, 4, 2, count, 8, 128), F32)
    whole = lambda shape: pl.BlockSpec(shape, lambda q: (0,) * len(shape))
    return pl.pallas_call(
        functools.partial(main_kernel, order=order),
        grid=(count,),
        in_specs=[
            whole((128, NP)), whole((NT, 64)), whole((subs, 2, NT, NP)),
            pl.BlockSpec((subs, 2, 1, 64, 128), lambda q: (0, 0, q + first, 0, 0)),
        ],
        out_specs=[pl.BlockSpec((4, 4, 2, 1, 8, 128), lambda q: (0, 0, 0, q, 0, 0))] * 2,
        out_shape=[out, out],
        name=f"main_{order}_{first}",
        cost_estimate=pl.CostEstimate(
            flops=count * 700_000_000, bytes_accessed=count * 2**19 + 2**21, transcendentals=0),
    )(uphi, utheta, table, pattern)


def split_kernel(me_ref, *refs, inputs):
    ins, outs = refs[:inputs], refs[inputs:]
    me = me_ref[0]
    for k, out in enumerate(outs):
        at = (me + k) % 4
        total = ins[0][at]
        for ref in ins[1:]:
            total = total + ref[at]
        out[...] = total


def split_call(me, arrays, name):
    shape = arrays[0].shape[1:]
    lead = shape[0]
    rest = shape[1:]
    steps = 4 if lead == 4 else 1
    block = (lead // steps,) + rest
    zeros = (0,) * len(rest)
    size = 4
    for d in shape:
        size *= d
    return pl.pallas_call(
        functools.partial(split_kernel, inputs=len(arrays)),
        grid=(steps,),
        in_specs=[pl.BlockSpec(memory_space=pltpu.SMEM)]
        + [pl.BlockSpec((4,) + block, lambda g: (0, g) + zeros)] * len(arrays),
        out_specs=[pl.BlockSpec(block, lambda g: (g,) + zeros)] * 4,
        out_shape=[jax.ShapeDtypeStruct(shape, F32)] * 4,
        name=name,
        cost_estimate=pl.CostEstimate(
            flops=size * len(arrays), bytes_accessed=4 * size * (len(arrays) + 1), transcendentals=0),
    )(me, *arrays)


def lane_group():
    return iota((8, 128), 1) // 32


def pack_kernel(me_ref, *refs, counts):
    ins, outs = refs[:-4], refs[-4:]
    me = me_ref[0]
    group = lane_group()
    places = []
    for c, (first, count) in enumerate(counts):
        for r in range(2):
            for q in range(count):
                places.append((r * 2 + (first + q) // 16, (first + q) % 16, c, r, q))
    tiles = {}
    for j, i, c, r, q in places:
        total = ins[4 * c][r, q]
        for n in range(1, 4):
            total = total + ins[4 * c + n][r, q]
        tiles[j, i] = total
    for i in range(16):
        for k in range(4):
            y = (me + k) % 4
            packed = None
            for j in range(4):
                moved = pltpu.roll(tiles[j, i], ((j + 4 - y) % 4) * 32, 1)
                packed = moved if packed is None else jnp.where(group == j, moved, packed)
            outs[k][i] = packed


def pack_call(me, arrays, counts):
    return pl.pallas_call(
        functools.partial(pack_kernel, counts=counts),
        in_specs=[pl.BlockSpec(memory_space=pltpu.SMEM)]
        + [pl.BlockSpec(memory_space=pltpu.VMEM)] * len(arrays),
        out_specs=[pl.BlockSpec(memory_space=pltpu.VMEM)] * 4,
        out_shape=[jax.ShapeDtypeStruct((16, 8, 128), F32)] * 4,
        name="pack",
    )(me, *arrays)


def root_kernel(a_ref, b_ref, c_ref, d_ref, root_ref, low_ref, high_ref):
    for i in range(16):
        root = (a_ref[i] + b_ref[i]) + (c_ref[i] + d_ref[i])
        root_ref[i] = root
        for k in range(2):
            low_ref[k, i:i + 1] = root[k:k + 1]
            high_ref[k, i:i + 1] = root[6 + k:7 + k]


def padded_rows(root_ref, low_ref, high_ref, i):
    return jnp.concatenate(
        [low_ref[0, i:i + 1], low_ref[1, i:i + 1], root_ref[i],
         high_ref[0, i:i + 1], high_ref[1, i:i + 1]], axis=0)


def edge_kernel(root_ref, low_ref, high_ref, left_ref, right_ref):
    place = iota((12, 128), 1) % 32 // 2
    left = jnp.zeros((12, 128), F32)
    right = jnp.zeros((12, 128), F32)
    for i in range(16):
        rows = padded_rows(root_ref, low_ref, high_ref, i)
        left = jnp.where(place == i, pltpu.roll(rows, 2 * i, 1) if i else rows, left)
        right = jnp.where(place == i, pltpu.roll(rows, (2 * i + 98) % 128, 1), right)
    left_ref[...] = left
    right_ref[...] = right


def weights_of(frac):
    p = 1.0 + frac
    return (
        -(p - 1.0) * (p - 2.0) * (p - 3.0) / 6.0,
        p * (p - 2.0) * (p - 3.0) / 2.0,
        -p * (p - 1.0) * (p - 3.0) / 2.0,
        p * (p - 1.0) * (p - 2.0) / 6.0,
    )


def field_kernel(band_ref, ts_ref, tf_ref, ps_ref, pf_ref, root_ref, low_ref, high_ref,
                 left_ref, right_ref, out_ref, *, subtrees):
    start = jnp.broadcast_to(ts_ref[...] - band_ref[0] * 8 + 2, (32, 128))
    taps = [jnp.broadcast_to(w, (32, 128)) for w in weights_of(tf_ref[...])]
    rows_w = []
    for t in range(12):
        w = jnp.zeros((32, 128), F32)
        for k in range(4):
            w = w + jnp.where(start + k == t, taps[k], 0.0)
        rows_w.append(w)

    def polar(rows):
        total = rows_w[0] * rows[0:1]
        for t in range(1, 12):
            total = total + rows_w[t] * rows[t:t + 1]
        return total

    lane = iota((128, NP), 0)
    pstart = ps_ref[...] - band_ref[1] * 32 + 2
    ptaps = weights_of(pf_ref[...])

    def phi_matrix(col):
        w = jnp.zeros((128, NP), F32)
        for k in range(4):
            w = w + jnp.where(col == pstart + k, ptaps[k], 0.0)
        return w

    matrix = jnp.concatenate(
        [phi_matrix(lane % 32 + 2), phi_matrix(lane % 2), phi_matrix(lane % 2 + 34)], axis=0)
    rim_left = polar(left_ref[...])
    rim_right = polar(right_ref[...])
    col = iota((32, 128), 1)
    for i in range(16):
        main = polar(padded_rows(root_ref, low_ref, high_ref, i))
        blocks = []
        for j in range(4):
            own = col // 32 == j
            rim = col // 2 == 16 * j + i
            blocks.append(jnp.concatenate(
                [jnp.where(own, main, 0.0), jnp.where(rim, rim_left, 0.0),
                 jnp.where(rim, rim_right, 0.0)], axis=1))
        field = jnp.dot(jnp.concatenate(blocks, axis=0), matrix,
                        precision=lax.Precision.HIGHEST, preferred_element_type=F32)
        power = field * field
        out_ref[i] = (power[0:32] + power[32:64] + power[64:96] + power[96:128]) * (1.0 / subtrees)


def exchanged(blocks, axis, size):
    out = [blocks[0]]
    for k in range(1, size):
        out.append(lax.ppermute(blocks[k], axis, [(i, (i + k) % size) for i in range(size)]))
    return out


def per_device(pattern, up_phi, up_theta, offsets, theta_start, theta_frac, phi_start, phi_frac):
    index = lambda axis: lax.axis_index(axis).astype(jnp.int32).reshape(1)
    subs = pattern.shape[0]
    vmem = pl.BlockSpec(memory_space=pltpu.VMEM)
    smem = pl.BlockSpec(memory_space=pltpu.SMEM)
    table, uphi, utheta = pl.pallas_call(
        prep_kernel,
        in_specs=[smem, smem, vmem, vmem],
        out_specs=[vmem] * 3,
        out_shape=[jax.ShapeDtypeStruct((subs, 2, NT, NP), F32),
                   jax.ShapeDtypeStruct((128, NP), BF16),
                   jax.ShapeDtypeStruct((NT, 64), BF16)],
        name="prep",
    )(index("c"), offsets, up_phi, up_theta)

    where = {"x": index("x"), "y": index("y"), "z": index(AXES["z"])}
    first_stage = {"x": [], "z": []}
    for order, first, count in CHUNKS:
        keep, send = main_call(order, first, count, uphi, utheta, table, pattern)
        other = lax.ppermute(send, "c", [(0, 1), (1, 0)])
        blocks = split_call(where[order], [keep, other], f"cut_{order}_{first}")
        first_stage[order].append((first, count, exchanged(blocks, AXES[order], 4)))

    pack_in, counts = [], []
    for order, then in (("x", "z"), ("z", "x")):
        for first, count, arrays in first_stage[order]:
            blocks = split_call(where[then], arrays, f"cut2_{order}_{first}")
            pack_in += exchanged(blocks, AXES[then], 4)
            counts.append((first, count))
    blocks = pack_call(where["y"], pack_in, tuple(counts))
    parts = exchanged(blocks, "y", 4)

    edge = jax.ShapeDtypeStruct((2, 16, 128), F32)
    root, low, high = pl.pallas_call(
        root_kernel,
        in_specs=[vmem] * 4,
        out_specs=[vmem] * 3,
        out_shape=[jax.ShapeDtypeStruct((16, 8, 128), F32), edge, edge],
        name="root",
    )(*parts)
    up = [(i, i + 1) for i in range(15)]
    below = lax.ppermute(high, THETA, up)
    above = lax.ppermute(low, THETA, [(b, a) for a, b in up])
    rim = jax.ShapeDtypeStruct((12, 128), F32)
    left, right = pl.pallas_call(
        edge_kernel, in_specs=[vmem] * 3, out_specs=[vmem] * 2, out_shape=[rim, rim], name="edges",
    )(root, below, above)
    ring = [(i, (i + 1) % 8) for i in range(8)]
    from_left = lax.ppermute(right, PHI, ring)
    from_right = lax.ppermute(left, PHI, [(b, a) for a, b in ring])

    band = jnp.stack([lax.axis_index(THETA), lax.axis_index(PHI)]).astype(jnp.int32)
    return pl.pallas_call(
        functools.partial(field_kernel, subtrees=float(subs * 128)),
        in_specs=[smem] + [vmem] * 9,
        out_specs=vmem,
        out_shape=jax.ShapeDtypeStruct((16, 32, NP), F32),
        name="field",
    )(band, theta_start.reshape(32, 1), theta_frac.reshape(32, 1), phi_start.reshape(1, NP),
      phi_frac.reshape(1, NP), root, below, above, from_left, from_right)


def solution(mesh):
    fine = Mesh(mesh.devices.reshape(4, 2, 4, 2, 2), ("y", "zh", "x", "zl", "c"))
    everyone = ("y", "zh", "x", "zl", "c")
    return jax.shard_map(
        per_device,
        mesh=fine,
        in_specs=(
            P(everyone, None, None, None, None), P(), P(), P(None, everyone),
            P(THETA), P(THETA), P(PHI), P(PHI),
        ),
        out_specs=P(None, THETA, PHI),
        check_vma=False,
    )
```

```python
import functools

import jax
import jax.numpy as jnp
from jax import lax
from jax.experimental import pallas as pl
from jax.experimental.pallas import tpu as pltpu
from jax.sharding import Mesh
from jax.sharding import PartitionSpec as P

NT = 128
NP = 256
F32 = jnp.float32
BF16 = jnp.bfloat16

CHUNKS = (("x", 0, 8), ("z", 16, 8), ("x", 8, 8), ("z", 24, 8))
AXES = {"x": "x", "z": ("zh", "zl"), "y": "y"}
THETA = ("x", "zl", "c")
PHI = ("y", "zh")

SIN = (6.283185005187988, -41.341590881347656, 81.59994506835938, -76.61446380615234,
       41.34282684326172, -12.47114372253418)
COS = (1.0, -19.73920440673828, 64.93911743164062, -85.45014190673828, 60.16762161254883,
       -25.96756935119629, 6.528613567352295)


def sincos_turns(turns):
    f = turns - jnp.round(turns)
    g = f * f
    s = jnp.full_like(g, SIN[-1])
    for coef in SIN[-2::-1]:
        s = s * g + coef
    c = jnp.full_like(g, COS[-1])
    for coef in COS[-2::-1]:
        c = c * g + coef
    return s * f, c


def vmem(shape, dtype=F32):
    return pltpu.VMEM(shape, dtype)


def held(*arrays):
    return [pltpu.with_memory_space_constraint(a, pltpu.VMEM) for a in arrays]


IN_VMEM = pl.BlockSpec(memory_space=pltpu.VMEM)
IN_SMEM = pl.BlockSpec(memory_space=pltpu.SMEM)
UNREAD = pl.BlockSpec(memory_space=pl.ANY)


def params(mib):
    return pltpu.CompilerParams(vmem_limit_bytes=mib * 2**20)


def iota(shape, dim):
    return lax.broadcasted_iota(jnp.int32, shape, dim)


def prep_kernel(core_ref, off_ref, uphi_ref, utheta_ref, table_ref, uphi_out, utheta_out):
    core = core_ref[0]
    row = iota((NT, NP), 0)
    theta = (row % 64) // 8 * 16 + ((row // 64) ^ core) * 8 + row % 8
    sin_t, cos_t = sincos_turns((theta.astype(F32) + 0.5) * (0.5 / NT))
    col = iota((NT, NP), 1)
    phi = (col % 128) // 32 * 64 + col // 128 * 32 + col % 32
    sin_p, cos_p = sincos_turns(phi.astype(F32) * (1.0 / NP))
    unit_x = sin_t * cos_p
    unit_y = sin_t * sin_p
    for s in range(table_ref.shape[0]):
        turns = off_ref[0, s] * unit_x + off_ref[1, s] * unit_y + off_ref[2, s] * cos_t
        sine, cosine = sincos_turns(turns)
        table_ref[s, 0] = cosine
        table_ref[s, 1] = sine
    src = iota((NP, NP), 0)
    dst = iota((NP, NP), 1)
    pick = ((dst % 128) // 32 * 64 + dst // 128 * 32 + dst % 32 == src).astype(F32).astype(BF16)
    uphi_out[...] = jnp.dot(uphi_ref[...], pick, preferred_element_type=F32).astype(BF16)
    r2 = iota((NT, NT), 0)
    th2 = (r2 % 64) // 8 * 16 + ((r2 // 64) ^ core) * 8 + r2 % 8
    pick2 = (iota((NT, NT), 1) == th2).astype(F32).astype(BF16)
    utheta_out[...] = lax.dot_general(
        pick2, utheta_ref[...], (((1,), (1,)), ((), ())), preferred_element_type=F32).astype(BF16)


def main_kernel(uphi_ref, utheta_ref, table_ref, pat_ref, *refs, order):
    keep_ref, send_ref = refs[-2:]
    subs, _, here = pat_ref.shape[:3]
    for n in range(here):
        q = pl.program_id(0) * here + n
        coarse = []
        for s in range(subs):
            both = pat_ref[s, :, n].reshape(128, 128)
            both = jnp.dot(both, uphi_ref[...], preferred_element_type=F32).astype(BF16)
            coarse.append(both.reshape(2, 64, NP))
        for half, out_ref in ((0, keep_ref), (1, send_ref)):
            rows = pl.ds(half * 64, 64)
            u = utheta_ref[rows, :]
            acc_r = jnp.zeros((64, NP), F32)
            acc_i = jnp.zeros((64, NP), F32)
            for s in range(subs):
                re = jnp.dot(u, coarse[s][0], preferred_element_type=F32)
                im = jnp.dot(u, coarse[s][1], preferred_element_type=F32)
                cosine = table_ref[s, 0, rows, :]
                sine = table_ref[s, 1, rows, :]
                acc_r = acc_r + (re * cosine - im * sine)
                acc_i = acc_i + (re * sine + im * cosine)
            for r, acc in ((0, acc_r), (1, acc_i)):
                for xi in range(4):
                    for zl in range(2):
                        tile = acc[(xi * 2 + zl) * 8:(xi * 2 + zl) * 8 + 8]
                        for zh in range(2):
                            zi = zh * 2 + zl
                            at = (xi, zi) if order == "x" else (zi, xi)
                            out_ref[at[0], at[1], r, q] = tile[:, zh * 128:zh * 128 + 128]


def main_call(order, first, count, uphi, utheta, table, pattern, after):
    subs = pattern.shape[0]
    here = 2
    out = vmem((4, 4, 2, count, 8, 128))
    return pl.pallas_call(
        functools.partial(main_kernel, order=order),
        grid=(count // here,),
        in_specs=[IN_VMEM] * 3 + [
            pl.BlockSpec((subs, 2, here, 64, 128), lambda g: (0, 0, g + first // here, 0, 0)),
        ] + [UNREAD] * len(after),
        out_specs=[IN_VMEM] * 2,
        out_shape=[out, out],
        compiler_params=params(16),
        name=f"main_{order}_{first}",
        cost_estimate=pl.CostEstimate(
            flops=count * 700_000_000, bytes_accessed=count * 2**19 + 2**21, transcendentals=0),
    )(*held(uphi, utheta, table), pattern, *held(*after))


def split_kernel(me_ref, *refs, group):
    ins, outs = refs[:-4], refs[-4:]
    me = me_ref[0]
    ahead = outs[0].ndim - 3
    for k, out in enumerate(outs):
        at = (me + k) % 4
        base = 0
        for n in range(0, len(ins), group):
            total = ins[n][at]
            for ref in ins[n + 1:n + group]:
                total = total + ref[at]
            count = total.shape[ahead]
            out[(slice(None),) * ahead + (slice(base, base + count),)] = total
            base += count


def split_call(me, groups, name):
    flat = [a for g in groups for a in g]
    lead = flat[0].shape[1:-3]
    count = sum(g[0].shape[-3] for g in groups)
    return pl.pallas_call(
        functools.partial(split_kernel, group=len(groups[0])),
        in_specs=[IN_SMEM] + [IN_VMEM] * len(flat),
        out_specs=[IN_VMEM] * 4,
        out_shape=[vmem(lead + (count, 8, 128))] * 4,
        compiler_params=params(4),
        name=name,
        cost_estimate=pl.CostEstimate(flops=10**6, bytes_accessed=0, transcendentals=0),
    )(me, *held(*flat))


def lane_group():
    return iota((8, 128), 1) // 32


def pack_kernel(me_ref, *refs, counts):
    ins, outs = refs[:-4], refs[-4:]
    me = me_ref[0]
    group = lane_group()
    places = []
    for c, channels in enumerate(counts):
        for r in range(2):
            for at, q in enumerate(channels):
                places.append((r * 2 + q // 16, q % 16, c, r, at))
    tiles = {}
    for j, i, c, r, q in places:
        total = ins[4 * c][r, q]
        for n in range(1, 4):
            total = total + ins[4 * c + n][r, q]
        tiles[j, i] = total
    for i in range(16):
        for k in range(4):
            y = (me + k) % 4
            packed = None
            for j in range(4):
                moved = pltpu.roll(tiles[j, i], ((j + 4 - y) % 4) * 32, 1)
                packed = moved if packed is None else jnp.where(group == j, moved, packed)
            outs[k][i] = packed


def pack_call(me, arrays, counts):
    return pl.pallas_call(
        functools.partial(pack_kernel, counts=counts),
        in_specs=[IN_SMEM] + [IN_VMEM] * len(arrays),
        out_specs=[IN_VMEM] * 4,
        out_shape=[vmem((16, 8, 128))] * 4,
        compiler_params=params(4),
        name="pack",
    )(me, *held(*arrays))


def root_kernel(a_ref, b_ref, c_ref, d_ref, root_ref, low_ref, high_ref):
    for i in range(16):
        root = (a_ref[i] + b_ref[i]) + (c_ref[i] + d_ref[i])
        root_ref[i] = root
        for k in range(2):
            low_ref[k, i:i + 1] = root[k:k + 1]
            high_ref[k, i:i + 1] = root[6 + k:7 + k]


def padded_rows(root_ref, low_ref, high_ref, i):
    return jnp.concatenate(
        [low_ref[0, i:i + 1], low_ref[1, i:i + 1], root_ref[i],
         high_ref[0, i:i + 1], high_ref[1, i:i + 1]], axis=0)


def edge_kernel(root_ref, low_ref, high_ref, left_ref, right_ref):
    place = iota((12, 128), 1) % 32 // 2
    left = jnp.zeros((12, 128), F32)
    right = jnp.zeros((12, 128), F32)
    for i in range(16):
        rows = padded_rows(root_ref, low_ref, high_ref, i)
        left = jnp.where(place == i, pltpu.roll(rows, 2 * i, 1) if i else rows, left)
        right = jnp.where(place == i, pltpu.roll(rows, (2 * i + 98) % 128, 1), right)
    left_ref[...] = left
    right_ref[...] = right


def weights_of(frac):
    p = 1.0 + frac
    return (
        -(p - 1.0) * (p - 2.0) * (p - 3.0) / 6.0,
        p * (p - 2.0) * (p - 3.0) / 2.0,
        -p * (p - 1.0) * (p - 3.0) / 2.0,
        p * (p - 1.0) * (p - 2.0) / 6.0,
    )


def halves(x):
    high = x.astype(BF16)
    return high, (x - high.astype(F32)).astype(BF16)


def field_kernel(band_ref, ts_ref, tf_ref, ps_ref, pf_ref, root_ref, low_ref, high_ref,
                 left_ref, right_ref, out_ref, *, subtrees):
    diagonal = iota((32, 32), 0) == iota((32, 32), 1)

    def column(row):
        return jnp.broadcast_to(
            jnp.sum(jnp.where(diagonal, row, 0.0), axis=1, keepdims=True), (32, 128))

    start = column((ts_ref[...] - band_ref[0] * 8 + 2).astype(F32))
    taps = weights_of(column(tf_ref[...]))
    rows_w = []
    for t in range(12):
        w = jnp.zeros((32, 128), F32)
        for k in range(4):
            w = w + jnp.where(start + k == t, taps[k], 0.0)
        rows_w.append(w)

    def polar(rows):
        total = rows_w[0] * rows[0:1]
        for t in range(1, 12):
            total = total + rows_w[t] * rows[t:t + 1]
        return total

    lane = iota((128, NP), 0)
    pstart = ps_ref[...] - band_ref[1] * 32 + 2
    ptaps = weights_of(pf_ref[...])

    def phi_matrix(col):
        w = jnp.zeros((128, NP), F32)
        for k in range(4):
            w = w + jnp.where(col == pstart + k, ptaps[k], 0.0)
        return w

    w_high, w_low = halves(jnp.concatenate(
        [phi_matrix(lane % 32 + 2), phi_matrix(lane % 2), phi_matrix(lane % 2 + 34)], axis=0))
    w_both = jnp.concatenate([w_high, w_high], axis=0)
    rims = halves(polar(left_ref[...])) + halves(polar(right_ref[...]))
    col = iota((32, 128), 1)
    zero = jnp.zeros((32, 128), F32)

    def masked(mask, value):
        return jnp.where(mask, value.astype(F32), zero).astype(BF16)

    for base in range(0, 16, 4):
        high, low = [], []
        for i in range(base, base + 4):
            main = halves(polar(padded_rows(root_ref, low_ref, high_ref, i)))
            for j in range(4):
                own = col // 32 == j
                rim = col // 2 == 16 * j + i
                for part, out in ((0, high), (1, low)):
                    out.append(jnp.concatenate(
                        [masked(own, main[part]), masked(rim, rims[part]),
                         masked(rim, rims[2 + part])], axis=1))
        high = jnp.concatenate(high, axis=0)
        low = jnp.concatenate(low, axis=0)
        field = jnp.dot(jnp.concatenate([high, low], axis=1), w_both,
                        preferred_element_type=F32)
        field = field + jnp.dot(high, w_low, preferred_element_type=F32)
        power = field * field
        for n in range(4):
            at = power[n * 128:n * 128 + 128]
            out_ref[base + n] = (
                (at[0:32] + at[32:64]) + (at[64:96] + at[96:128])) * (1.0 / subtrees)


def exchanged(blocks, axis, size):
    out = [blocks[0]]
    for k in range(1, size):
        out.append(lax.ppermute(blocks[k], axis, [(i, (i + k) % size) for i in range(size)]))
    return out


def per_device(pattern, up_phi, up_theta, offsets, theta_start, theta_frac, phi_start, phi_frac):
    index = lambda axis: lax.axis_index(axis).astype(jnp.int32).reshape(1)
    subs = pattern.shape[0]
    table, uphi, utheta = pl.pallas_call(
        prep_kernel,
        in_specs=[IN_SMEM, IN_SMEM, IN_VMEM, IN_VMEM],
        out_specs=[IN_VMEM] * 3,
        out_shape=[vmem((subs, 2, NT, NP)), vmem((128, NP), BF16), vmem((NT, 64), BF16)],
        compiler_params=params(8),
        name="prep",
    )(index("c"), offsets, *held(up_phi, up_theta.T))

    where = {"x": index("x"), "y": index("y"), "z": index(AXES["z"])}
    first_stage = {"x": [], "z": []}
    waiting = []
    after = []

    def first_cut():
        order, first, count, keep, other = waiting.pop(0)
        blocks = split_call(where[order], [[keep, other]], f"cut_{order}_{first}")
        first_stage[order].append((first, count, exchanged(blocks, AXES[order], 4)))
        return [blocks[0]]

    for order, first, count in CHUNKS:
        keep, send = main_call(order, first, count, uphi, utheta, table, pattern, after)
        other = lax.ppermute(send, "c", [(0, 1), (1, 0)])
        waiting.append((order, first, count, keep, other))
        after = first_cut() if len(waiting) == 2 else []
    first_cut()

    pack_in, counts = [], []
    for order, then in (("x", "z"), ("z", "x")):
        chunks = first_stage[order]
        blocks = split_call(where[then], [c[2] for c in chunks], f"cut2_{order}")
        pack_in += exchanged(blocks, AXES[then], 4)
        counts.append(tuple(q for first, count, _ in chunks for q in range(first, first + count)))
    blocks = pack_call(where["y"], pack_in, tuple(counts))
    parts = exchanged(blocks, "y", 4)

    edge = vmem((2, 16, 128))
    root, low, high = pl.pallas_call(
        root_kernel,
        in_specs=[IN_VMEM] * 4,
        out_specs=[IN_VMEM] * 3,
        out_shape=[vmem((16, 8, 128)), edge, edge],
        compiler_params=params(4),
        name="root",
    )(*held(*parts))
    up = [(i, i + 1) for i in range(15)]
    below = lax.ppermute(high, THETA, up)
    above = lax.ppermute(low, THETA, [(b, a) for a, b in up])
    left, right = pl.pallas_call(
        edge_kernel, in_specs=[IN_VMEM] * 3, out_specs=[IN_VMEM] * 2,
        out_shape=[vmem((12, 128))] * 2, compiler_params=params(4), name="edges",
    )(*held(root, below, above))
    ring = [(i, (i + 1) % 8) for i in range(8)]
    from_left = lax.ppermute(right, PHI, ring)
    from_right = lax.ppermute(left, PHI, [(b, a) for a, b in ring])

    band = jnp.stack([lax.axis_index(THETA), lax.axis_index(PHI)]).astype(jnp.int32)
    return pl.pallas_call(
        functools.partial(field_kernel, subtrees=float(subs * 128)),
        in_specs=[IN_SMEM] + [IN_VMEM] * 9,
        out_specs=IN_VMEM,
        out_shape=jax.ShapeDtypeStruct((16, 32, NP), F32),
        compiler_params=params(16),
        name="field",
    )(band, *held(theta_start.reshape(1, 32), theta_frac.reshape(1, 32), phi_start.reshape(1, NP),
                  phi_frac.reshape(1, NP), root, below, above, from_left, from_right))


def solution(mesh):
    fine = Mesh(mesh.devices.reshape(4, 2, 4, 2, 2), ("y", "zh", "x", "zl", "c"))
    everyone = ("y", "zh", "x", "zl", "c")
    return jax.shard_map(
        per_device,
        mesh=fine,
        in_specs=(
            P(everyone, None, None, None, None), P(), P(), P(None, everyone),
            P(THETA), P(THETA), P(PHI), P(PHI),
        ),
        out_specs=P(None, THETA, PHI),
        check_vma=False,
    )
```

```python
import functools

import jax
import jax.numpy as jnp
from jax import lax
from jax.experimental import pallas as pl
from jax.experimental.pallas import tpu as pltpu
from jax.sharding import Mesh
from jax.sharding import PartitionSpec as P


NT = 128
NP = 256
F32 = jnp.float32
BF16 = jnp.bfloat16

CHUNKS = (('x', 0, 12), ('z', 16, 12), ('x', 12, 4), ('z', 28, 4))
AXES = {"x": "x", "z": ("zh", "zl"), "y": "y"}
PLACES = ("c", "x", "y", "z", "theta", "phi")
THETA = ("x", "zl", "c")
PHI = ("y", "zh")

SIN = (6.283185005187988, -41.341590881347656, 81.59994506835938, -76.61446380615234,
       41.34282684326172, -12.47114372253418)
COS = (1.0, -19.73920440673828, 64.93911743164062, -85.45014190673828, 60.16762161254883,
       -25.96756935119629, 6.528613567352295)


def sincos_turns(turns):
    f = turns - jnp.round(turns)
    g = f * f
    s = jnp.full_like(g, SIN[-1])
    for coef in SIN[-2::-1]:
        s = s * g + coef
    c = jnp.full_like(g, COS[-1])
    for coef in COS[-2::-1]:
        c = c * g + coef
    return s * f, c


def vmem(shape, dtype=F32):
    return pltpu.VMEM(shape, dtype)


def in_hbm(*arrays):
    return [pltpu.with_memory_space_constraint(a, pltpu.HBM) for a in arrays]


def held(*arrays):
    return [pltpu.with_memory_space_constraint(a, pltpu.VMEM) for a in arrays]


IN_VMEM = pl.BlockSpec(memory_space=pltpu.VMEM)
IN_SMEM = pl.BlockSpec(memory_space=pltpu.SMEM)
UNREAD = pl.BlockSpec(memory_space=pl.ANY)


def params(mib):
    return pltpu.CompilerParams(vmem_limit_bytes=mib * 2**20)


def iota(shape, dim):
    return lax.broadcasted_iota(jnp.int32, shape, dim)


def prep_kernel(place_ref, off_ref, uphi_ref, utheta_ref, table_ref, uphi_out, utheta_out):
    core = place_ref[PLACES.index("c")]
    row = iota((NT, NP), 0)
    theta = (row % 64) // 8 * 16 + ((row // 64) ^ core) * 8 + row % 8
    sin_t, cos_t = sincos_turns((theta.astype(F32) + 0.5) * (0.5 / NT))
    col = iota((NT, NP), 1)
    phi = (col % 128) // 32 * 64 + col // 128 * 32 + col % 32
    sin_p, cos_p = sincos_turns(phi.astype(F32) * (1.0 / NP))
    unit_x = sin_t * cos_p
    unit_y = sin_t * sin_p
    for s in range(table_ref.shape[0]):
        turns = off_ref[0, s] * unit_x + off_ref[1, s] * unit_y + off_ref[2, s] * cos_t
        sine, cosine = sincos_turns(turns)
        table_ref[s, 0] = cosine
        table_ref[s, 1] = sine
    src = iota((NP, NP), 0)
    dst = iota((NP, NP), 1)
    pick = ((dst % 128) // 32 * 64 + dst // 128 * 32 + dst % 32 == src).astype(F32).astype(BF16)
    uphi_out[...] = jnp.dot(uphi_ref[...], pick, preferred_element_type=F32).astype(BF16)
    r2 = iota((NT, NT), 0)
    th2 = (r2 % 64) // 8 * 16 + ((r2 // 64) ^ core) * 8 + r2 % 8
    pick2 = (iota((NT, NT), 1) == th2).astype(F32).astype(BF16)
    utheta_out[...] = lax.dot_general(
        pick2, utheta_ref[...], (((1,), (1,)), ((), ())), preferred_element_type=F32).astype(BF16)


def main_kernel(uphi_ref, utheta_ref, table_ref, pat_ref, *refs, order):
    keep_ref, send_ref = refs[-2:]
    subs, _, here = pat_ref.shape[:3]
    count = keep_ref.shape[2] // 2
    for n in range(here):
        q = pl.program_id(0) * here + n
        coarse = []
        for s in range(subs):
            both = pat_ref[s, :, n].reshape(128, 128)
            both = jnp.dot(both, uphi_ref[...], preferred_element_type=F32).astype(BF16)
            coarse.append(both.reshape(2, 64, NP))
        for half, out_ref in ((0, keep_ref), (1, send_ref)):
            rows = pl.ds(half * 64, 64)
            u = utheta_ref[rows, :]
            acc_r = jnp.zeros((64, NP), F32)
            acc_i = jnp.zeros((64, NP), F32)
            for s in range(subs):
                re = jnp.dot(u, coarse[s][0], preferred_element_type=F32)
                im = jnp.dot(u, coarse[s][1], preferred_element_type=F32)
                cosine = table_ref[s, 0, rows, :]
                sine = table_ref[s, 1, rows, :]
                acc_r = acc_r + (re * cosine - im * sine)
                acc_i = acc_i + (re * sine + im * cosine)
            for r, acc in ((0, acc_r), (1, acc_i)):
                for xi in range(4):
                    for zl in range(2):
                        tile = acc[(xi * 2 + zl) * 8:(xi * 2 + zl) * 8 + 8]
                        for zh in range(2):
                            zi = zh * 2 + zl
                            at = (xi, zi) if order == "x" else (zi, xi)
                            out_ref[at[0], at[1], r * count + q] = tile[:, zh * 128:zh * 128 + 128]


def main_call(order, first, count, uphi, utheta, table, pattern, after):
    subs = pattern.shape[0]
    here = 4
    out = vmem((4, 4, 2 * count, 8, 128))
    return pl.pallas_call(
        functools.partial(main_kernel, order=order),
        grid=(count // here,),
        in_specs=[IN_VMEM] * 3 + [
            pl.BlockSpec((subs, 2, here, 64, 128), lambda g: (0, 0, g + first // here, 0, 0)),
        ] + [UNREAD] * len(after),
        out_specs=[IN_VMEM] * 2,
        out_shape=[out, out],
        compiler_params=params(16),
        cost_estimate=pl.CostEstimate(
            flops=count * 700_000_000, bytes_accessed=count * 2**19 + 2**21, transcendentals=0),
    )(*held(uphi, utheta, table), *in_hbm(pattern), *held(*after))


def split_kernel(place_ref, *refs, axis, group, rims):
    ins, outs = refs[:-4], refs[-4:]
    me = place_ref[PLACES.index(axis)]
    slot_of = iota((8, 128), 1) % 32 // 4
    for k, out in enumerate(outs):
        at = (me + k) % 4

        def total(n, index):
            value = ins[n][index]
            for ref in ins[n + 1:n + group]:
                value = value + ref[index]
            return value

        base = 0
        for n in range(0, len(ins), group):
            shape = ins[n].shape
            tiles = shape[-3]
            for outer in range(shape[1]) if len(shape) == 5 else (None,):
                lead = () if outer is None else (outer,)
                out[lead + (slice(base, base + tiles),)] = total(n, (at,) + lead)
                if not rims:
                    continue
                other = at ^ 2
                shift = jnp.where(at < 2, 2, 98)
                for first in range(0, tiles, 8):
                    rim = jnp.zeros((8, 128), F32)
                    for slot in range(8):
                        tile = total(n, (other,) + lead + (first + slot,))
                        moved = pltpu.roll(tile, (shift + 4 * slot) % 128, 1)
                        rim = jnp.where(slot_of == slot, moved, rim)
                    out[lead + (base + tiles + first // 8,)] = rim
            base += tiles + (tiles // 8 if rims else 0)


def split_call(place, axis, groups):
    flat = [a for g in groups for a in g]
    lead = flat[0].shape[1:-3]
    count = sum(g[0].shape[-3] for g in groups)
    rims = axis == "z"
    count += count // 8 if rims else 0
    return pl.pallas_call(
        functools.partial(split_kernel, axis=axis, group=len(groups[0]), rims=rims),
        in_specs=[IN_SMEM] + [IN_VMEM] * len(flat),
        out_specs=[IN_VMEM] * 4,
        out_shape=[vmem(lead + (count, 8, 128))] * 4,
        compiler_params=params(4),
        cost_estimate=pl.CostEstimate(flops=10**6, bytes_accessed=0, transcendentals=0),
    )(place, *held(*flat))


def lane_group():
    return iota((8, 128), 1) // 32


def places_of(orders):
    tiles, rims = {}, []
    for o, chunks in enumerate(orders):
        base = 0
        for first, count in chunks:
            for t in range(2 * count):
                r, q = t // count, first + t % count
                rim = len(rims) + t // 8
                tiles[2 * r + q // 16, q % 16] = (o, base + t, rim, t % 8)
            rims += [(o, base + 2 * count + n) for n in range(count // 4)]
            base += 2 * count + count // 4
    return tiles, rims


def pack_kernel(place_ref, *refs, orders):
    ins, outs = refs[:-4], refs[-4:]
    me = place_ref[PLACES.index("y")]
    group = lane_group()
    tiles, rims = places_of(orders)

    def total(o, t):
        return (ins[4 * o][t] + ins[4 * o + 1][t]) + (ins[4 * o + 2][t] + ins[4 * o + 3][t])

    for i in range(18):
        if i < 16:
            four = [total(*tiles[j, i][:2]) for j in range(4)]
        else:
            four = [total(*rims[(i - 16) * 4 + j]) for j in range(4)]
        for k in range(4):
            y = (me + k) % 4
            packed = None
            for j in range(4):
                moved = pltpu.roll(four[j], ((j + 4 - y) % 4) * 32, 1)
                packed = moved if packed is None else jnp.where(group == j, moved, packed)
            outs[k][i] = packed


def pack_call(place, arrays, orders):
    return pl.pallas_call(
        functools.partial(pack_kernel, orders=orders),
        in_specs=[IN_SMEM] + [IN_VMEM] * len(arrays),
        out_specs=[IN_VMEM] * 4,
        out_shape=[vmem((18, 8, 128))] * 4,
        compiler_params=params(4),
        name="pack",
    )(place, *held(*arrays))


def root_kernel(a_ref, b_ref, c_ref, d_ref, root_ref, low_ref, high_ref):
    for i in range(18):
        root = (a_ref[i] + b_ref[i]) + (c_ref[i] + d_ref[i])
        root_ref[i] = root
        for k in range(2):
            low_ref[k, i:i + 1] = root[k:k + 1]
            high_ref[k, i:i + 1] = root[6 + k:7 + k]


def padded_rows(root_ref, low_ref, high_ref, i):
    return jnp.concatenate(
        [low_ref[0, i:i + 1], low_ref[1, i:i + 1], root_ref[i],
         high_ref[0, i:i + 1], high_ref[1, i:i + 1]], axis=0)


def weights_of(frac):
    p = 1.0 + frac
    return (
        -(p - 1.0) * (p - 2.0) * (p - 3.0) / 6.0,
        p * (p - 2.0) * (p - 3.0) / 2.0,
        -p * (p - 1.0) * (p - 3.0) / 2.0,
        p * (p - 1.0) * (p - 2.0) / 6.0,
    )


def halves(x):
    high = x.astype(BF16)
    return high, (x - high.astype(F32)).astype(BF16)


def field_kernel(place_ref, ts_ref, tf_ref, ps_ref, pf_ref, root_ref, low_ref, high_ref,
                 out_ref, *, subtrees, orders):
    diagonal = iota((32, 32), 0) == iota((32, 32), 1)

    def column(row):
        return jnp.broadcast_to(
            jnp.sum(jnp.where(diagonal, row, 0.0), axis=1, keepdims=True), (32, 128))

    start = column((ts_ref[...] - place_ref[PLACES.index("theta")] * 8 + 2).astype(F32))
    taps = weights_of(column(tf_ref[...]))
    rows_w = []
    for t in range(12):
        w = jnp.zeros((32, 128), F32)
        for k in range(4):
            w = w + jnp.where(start + k == t, taps[k], 0.0)
        rows_w.append(w)

    def polar(rows):
        total = rows_w[0] * rows[0:1]
        for t in range(1, 12):
            total = total + rows_w[t] * rows[t:t + 1]
        return total

    lane = iota((128, NP), 0)
    pstart = ps_ref[...] - place_ref[PLACES.index("phi")] * 32 + 2
    ptaps = weights_of(pf_ref[...])

    def phi_matrix(col):
        w = jnp.zeros((128, NP), F32)
        for k in range(4):
            w = w + jnp.where(col == pstart + k, ptaps[k], 0.0)
        return w

    side = lane % 4
    w_high, w_low = halves(jnp.concatenate(
        [phi_matrix(lane % 32 + 2), phi_matrix(jnp.where(side < 2, side, side + 32))], axis=0))
    w_both = jnp.concatenate([w_high, w_high], axis=0)
    tiles, _ = places_of(orders)
    rims = [halves(polar(padded_rows(root_ref, low_ref, high_ref, 16 + p))) for p in range(2)]
    col = iota((32, 128), 1)
    zero = jnp.zeros((32, 128), F32)

    def masked(mask, value):
        return jnp.where(mask, value.astype(F32), zero).astype(BF16)

    for base in range(0, 16, 4):
        high, low = [], []
        for i in range(base, base + 4):
            main = halves(polar(padded_rows(root_ref, low_ref, high_ref, i)))
            for j in range(4):
                _, _, rim_tile, slot = tiles[j, i]
                own = col // 32 == j
                rim = col // 4 == rim_tile % 4 * 8 + slot
                for part, out in ((0, high), (1, low)):
                    out.append(jnp.concatenate(
                        [masked(own, main[part]), masked(rim, rims[rim_tile // 4][part])], axis=1))
        high = jnp.concatenate(high, axis=0)
        low = jnp.concatenate(low, axis=0)
        field = jnp.dot(jnp.concatenate([high, low], axis=1), w_both,
                        preferred_element_type=F32)
        field = field + jnp.dot(high, w_low, preferred_element_type=F32)
        power = field * field
        for n in range(4):
            at = power[n * 128:n * 128 + 128]
            out_ref[base + n] = (
                (at[0:32] + at[32:64]) + (at[64:96] + at[96:128])) * (1.0 / subtrees)


def exchanged(blocks, axis, size):
    out = [blocks[0]]
    for k in range(1, size):
        out.append(lax.ppermute(blocks[k], axis, [(i, (i + k) % size) for i in range(size)]))
    return out


def per_device(pattern, up_phi, up_theta, offsets, theta_start, theta_frac, phi_start, phi_frac):
    axes = ("c", "x", "y", AXES["z"], THETA, PHI)
    place = jnp.stack([lax.axis_index(a) for a in axes]).astype(jnp.int32)
    subs = pattern.shape[0]
    table, uphi, utheta = pl.pallas_call(
        prep_kernel,
        in_specs=[IN_SMEM, IN_SMEM, IN_VMEM, IN_VMEM],
        out_specs=[IN_VMEM] * 3,
        out_shape=[vmem((subs, 2, NT, NP)), vmem((128, NP), BF16), vmem((NT, 64), BF16)],
        compiler_params=params(8),
        name="prep",
    )(place, *in_hbm(offsets, up_phi, up_theta.T))

    first_stage = {"x": [], "z": []}
    waiting = []
    after = []

    def first_cut():
        order, first, count, keep, other = waiting.pop(0)
        blocks = split_call(place, order, [[keep, other]])
        arrays = exchanged(blocks, AXES[order], 4)
        first_stage[order].append((first, count, arrays))
        return [blocks[0]]

    for order, first, count in CHUNKS:
        keep, send = main_call(order, first, count, uphi, utheta, table, pattern, after)
        other = lax.ppermute(send, "c", [(0, 1), (1, 0)])
        waiting.append((order, first, count, keep, other))
        after = first_cut() if len(waiting) == 2 else []
    first_cut()

    pack_in, orders = [], []
    for order, then in (("x", "z"), ("z", "x")):
        chunks = first_stage[order]
        blocks = split_call(place, then, [c[2] for c in chunks])
        pack_in += exchanged(blocks, AXES[then], 4)
        orders.append(tuple(c[:2] for c in chunks))
    orders = tuple(orders)
    blocks = pack_call(place, pack_in, orders)
    parts = exchanged(blocks, "y", 4)

    edge = vmem((2, 18, 128))
    root, low, high = pl.pallas_call(
        root_kernel,
        in_specs=[IN_VMEM] * 4,
        out_specs=[IN_VMEM] * 3,
        out_shape=[vmem((18, 8, 128)), edge, edge],
        compiler_params=params(4),
        name="root",
    )(*held(*parts))
    up = [(i, i + 1) for i in range(15)]
    below = lax.ppermute(high, THETA, up)
    above = lax.ppermute(low, THETA, [(b, a) for a, b in up])

    return pl.pallas_call(
        functools.partial(field_kernel, subtrees=float(subs * 128), orders=orders),
        in_specs=[IN_SMEM] + [IN_VMEM] * 7,
        out_specs=IN_VMEM,
        out_shape=jax.ShapeDtypeStruct((16, 32, NP), F32),
        compiler_params=params(16),
        name="field",
    )(place, *in_hbm(theta_start.reshape(1, 32), theta_frac.reshape(1, 32),
                    phi_start.reshape(1, NP), phi_frac.reshape(1, NP)),
      *held(root, below, above))


def solution(mesh):
    fine = Mesh(mesh.devices.reshape(4, 2, 4, 2, 2), ("y", "zh", "x", "zl", "c"))
    everyone = ("y", "zh", "x", "zl", "c")

    return jax.shard_map(
        per_device,
        mesh=fine,
        in_specs=(
            P(everyone, None, None, None, None), P(), P(), P(None, everyone),
            P(THETA), P(THETA), P(PHI), P(PHI),
        ),
        out_specs=P(None, THETA, PHI),
        check_vma=False,
    )
```

```python
import functools

import jax
import jax.numpy as jnp
from jax import lax
from jax.experimental import pallas as pl
from jax.experimental.pallas import tpu as pltpu
from jax.sharding import Mesh
from jax.sharding import PartitionSpec as P


NT = 128
NP = 256
F32 = jnp.float32
BF16 = jnp.bfloat16

CHUNKS = (('x', 0, 12), ('z', 20, 8), ('x', 12, 8), ('z', 28, 4))
GROUP = 4
AXES = {"x": "x", "z": ("zh", "zl"), "y": "y"}
PLACES = ("c", "x", "y", "z", "theta", "phi")
THETA = ("x", "zl", "c")
PHI = ("y", "zh")

SIN = (6.283185005187988, -41.341590881347656, 81.59994506835938, -76.61446380615234,
       41.34282684326172, -12.47114372253418)
COS = (1.0, -19.73920440673828, 64.93911743164062, -85.45014190673828, 60.16762161254883,
       -25.96756935119629, 6.528613567352295)


def sincos_turns(turns):
    f = turns - jnp.round(turns)
    g = f * f
    s = jnp.full_like(g, SIN[-1])
    for coef in SIN[-2::-1]:
        s = s * g + coef
    c = jnp.full_like(g, COS[-1])
    for coef in COS[-2::-1]:
        c = c * g + coef
    return s * f, c


def vmem(shape, dtype=F32):
    return pltpu.VMEM(shape, dtype)


def in_hbm(*arrays):
    return [pltpu.with_memory_space_constraint(a, pltpu.HBM) for a in arrays]


def held(*arrays):
    return [pltpu.with_memory_space_constraint(a, pltpu.VMEM) for a in arrays]


IN_VMEM = pl.BlockSpec(memory_space=pltpu.VMEM)
IN_HBM = pl.BlockSpec(memory_space=pltpu.HBM)
IN_SMEM = pl.BlockSpec(memory_space=pltpu.SMEM)
UNREAD = pl.BlockSpec(memory_space=pl.ANY)


def params(mib):
    return pltpu.CompilerParams(vmem_limit_bytes=mib * 2**20)


def iota(shape, dim):
    return lax.broadcasted_iota(jnp.int32, shape, dim)


def fetch(pat_ref, first, dst_ref, sem):
    return pltpu.make_async_copy(pat_ref.at[:, :, pl.ds(first, GROUP)], dst_ref, sem)


def prep_kernel(place_ref, off_ref, uphi_ref, utheta_ref, pat_ref, table_ref, uphi_out, utheta_out,
                next_ref, sem):
    ahead = fetch(pat_ref, CHUNKS[0][1], next_ref, sem.at[0])
    ahead.start()
    core = place_ref[PLACES.index("c")]
    row = iota((NT, NP), 0)
    theta = (row % 64) // 8 * 16 + ((row // 64) ^ core) * 8 + row % 8
    sin_t, cos_t = sincos_turns((theta.astype(F32) + 0.5) * (0.5 / NT))
    col = iota((NT, NP), 1)
    phi = (col % 128) // 32 * 64 + col // 128 * 32 + col % 32
    sin_p, cos_p = sincos_turns(phi.astype(F32) * (1.0 / NP))
    unit_x = sin_t * cos_p
    unit_y = sin_t * sin_p
    for s in range(table_ref.shape[0]):
        turns = off_ref[0, s] * unit_x + off_ref[1, s] * unit_y + off_ref[2, s] * cos_t
        sine, cosine = sincos_turns(turns)
        table_ref[s, 0] = cosine
        table_ref[s, 1] = sine
    src = iota((NP, NP), 0)
    dst = iota((NP, NP), 1)
    pick = ((dst % 128) // 32 * 64 + dst // 128 * 32 + dst % 32 == src).astype(F32).astype(BF16)
    uphi_out[...] = jnp.dot(uphi_ref[...], pick, preferred_element_type=F32).astype(BF16)
    r2 = iota((NT, NT), 0)
    th2 = (r2 % 64) // 8 * 16 + ((r2 // 64) ^ core) * 8 + r2 % 8
    pick2 = (iota((NT, NT), 1) == th2).astype(F32).astype(BF16)
    utheta_out[...] = lax.dot_general(
        pick2, utheta_ref[...], (((1,), (1,)), ((), ())), preferred_element_type=F32).astype(BF16)
    ahead.wait()


def main_kernel(uphi_ref, utheta_ref, table_ref, part_ref, whole_ref, *refs, order, first,
                following):
    own, sem = refs[-2:]
    keep_ref, send_ref = refs[-4 - (following is not None):][:2]
    subs, _, count = own.shape[:3]
    groups = count // GROUP
    for g in range(1, groups):
        fetch(whole_ref, first + g * GROUP, own.at[:, :, pl.ds(g * GROUP, GROUP)], sem.at[g]).start()
    if following is not None:
        ahead = fetch(whole_ref, following[1], refs[-3], sem.at[0])
        ahead.start()
    own[:, :, 0:GROUP] = part_ref[...]

    def channel(q):
        coarse = []
        for s in range(subs):
            both = own[s, :, q].reshape(128, 128)
            both = jnp.dot(both, uphi_ref[...], preferred_element_type=F32).astype(BF16)
            coarse.append(both.reshape(2, 64, NP))
        for half, out_ref in ((0, keep_ref), (1, send_ref)):
            rows = pl.ds(half * 64, 64)
            u = utheta_ref[rows, :]
            acc_r = jnp.zeros((64, NP), F32)
            acc_i = jnp.zeros((64, NP), F32)
            for s in range(subs):
                re = jnp.dot(u, coarse[s][0], preferred_element_type=F32)
                im = jnp.dot(u, coarse[s][1], preferred_element_type=F32)
                cosine = table_ref[s, 0, rows, :]
                sine = table_ref[s, 1, rows, :]
                acc_r = acc_r + (re * cosine - im * sine)
                acc_i = acc_i + (re * sine + im * cosine)
            for r, acc in ((0, acc_r), (1, acc_i)):
                for xi in range(4):
                    for zl in range(2):
                        tile = acc[(xi * 2 + zl) * 8:(xi * 2 + zl) * 8 + 8]
                        for zh in range(2):
                            zi = zh * 2 + zl
                            at = (xi, zi) if order == "x" else (zi, xi)
                            out_ref[at[0], at[1], r * count + q] = tile[:, zh * 128:zh * 128 + 128]

    @pl.loop(0, groups)
    def _(g):
        @pl.when(g > 0)
        def _():
            fetch(whole_ref, first + g * GROUP, own.at[:, :, pl.ds(g * GROUP, GROUP)],
                  sem.at[g]).wait()

        for n in range(GROUP):
            channel(g * GROUP + n)

    if following is not None:
        ahead.wait()


def main_call(chunk, following, uphi, utheta, table, part, pattern, after):
    order, first, count = chunk
    subs = pattern.shape[0]
    out = vmem((4, 4, 2 * count, 8, 128))
    more = following is not None
    outs = pl.pallas_call(
        functools.partial(main_kernel, order=order, first=first, following=following),
        in_specs=[IN_VMEM] * 4 + [IN_HBM] + [UNREAD] * len(after),
        out_specs=[IN_VMEM] * (2 + more),
        out_shape=[out, out] + [vmem((subs, 2, GROUP, 64, 128), BF16)] * more,
        scratch_shapes=[vmem((subs, 2, count, 64, 128), BF16),
                        pltpu.SemaphoreType.DMA((count // GROUP,))],
        compiler_params=params(10),
        cost_estimate=pl.CostEstimate(
            flops=count * 700_000_000, bytes_accessed=count * 2**19 + 2**21, transcendentals=0),
    )(*held(uphi, utheta, table, part), *in_hbm(pattern), *held(*after))
    return outs if more else (*outs, None)


def split_kernel(place_ref, *refs, axis, group, rims):
    ins, outs = refs[:-4], refs[-4:]
    me = place_ref[PLACES.index(axis)]
    slot_of = iota((8, 128), 1) % 32 // 4
    for k, out in enumerate(outs):
        at = (me + k) % 4

        def total(n, index):
            value = ins[n][index]
            for ref in ins[n + 1:n + group]:
                value = value + ref[index]
            return value

        base = 0
        for n in range(0, len(ins), group):
            shape = ins[n].shape
            tiles = shape[-3]
            for outer in range(shape[1]) if len(shape) == 5 else (None,):
                lead = () if outer is None else (outer,)
                out[lead + (slice(base, base + tiles),)] = total(n, (at,) + lead)
                if not rims:
                    continue
                other = at ^ 2
                shift = jnp.where(at < 2, 2, 98)
                for first in range(0, tiles, 8):
                    rim = jnp.zeros((8, 128), F32)
                    for slot in range(8):
                        tile = total(n, (other,) + lead + (first + slot,))
                        moved = pltpu.roll(tile, (shift + 4 * slot) % 128, 1)
                        rim = jnp.where(slot_of == slot, moved, rim)
                    out[lead + (base + tiles + first // 8,)] = rim
            base += tiles + (tiles // 8 if rims else 0)


def split_call(place, axis, groups):
    flat = [a for g in groups for a in g]
    lead = flat[0].shape[1:-3]
    count = sum(g[0].shape[-3] for g in groups)
    rims = axis == "z"
    count += count // 8 if rims else 0
    return pl.pallas_call(
        functools.partial(split_kernel, axis=axis, group=len(groups[0]), rims=rims),
        in_specs=[IN_SMEM] + [IN_VMEM] * len(flat),
        out_specs=[IN_VMEM] * 4,
        out_shape=[vmem(lead + (count, 8, 128))] * 4,
        compiler_params=params(4),
        cost_estimate=pl.CostEstimate(flops=10**6, bytes_accessed=0, transcendentals=0),
    )(place, *held(*flat))


def lane_group():
    return iota((8, 128), 1) // 32


def places_of(orders):
    tiles, rims = {}, []
    for o, chunks in enumerate(orders):
        base = 0
        for first, count in chunks:
            for t in range(2 * count):
                r, q = t // count, first + t % count
                rim = len(rims) + t // 8
                tiles[2 * r + q // 16, q % 16] = (o, base + t, rim, t % 8)
            rims += [(o, base + 2 * count + n) for n in range(count // 4)]
            base += 2 * count + count // 4
    return tiles, rims


def pack_kernel(place_ref, *refs, orders):
    ins, outs = refs[:-4], refs[-4:]
    me = place_ref[PLACES.index("y")]
    group = lane_group()
    tiles, rims = places_of(orders)

    def total(o, t):
        return (ins[4 * o][t] + ins[4 * o + 1][t]) + (ins[4 * o + 2][t] + ins[4 * o + 3][t])

    for i in range(18):
        if i < 16:
            four = [total(*tiles[j, i][:2]) for j in range(4)]
        else:
            four = [total(*rims[(i - 16) * 4 + j]) for j in range(4)]
        for k in range(4):
            y = (me + k) % 4
            packed = None
            for j in range(4):
                moved = pltpu.roll(four[j], ((j + 4 - y) % 4) * 32, 1)
                packed = moved if packed is None else jnp.where(group == j, moved, packed)
            outs[k][i] = packed


def pack_call(place, arrays, orders):
    return pl.pallas_call(
        functools.partial(pack_kernel, orders=orders),
        in_specs=[IN_SMEM] + [IN_VMEM] * len(arrays),
        out_specs=[IN_VMEM] * 4,
        out_shape=[vmem((18, 8, 128))] * 4,
        compiler_params=params(4),
        name="pack",
    )(place, *held(*arrays))


def root_kernel(a_ref, b_ref, c_ref, d_ref, root_ref, low_ref, high_ref):
    for i in range(18):
        root = (a_ref[i] + b_ref[i]) + (c_ref[i] + d_ref[i])
        root_ref[i] = root
        for k in range(2):
            low_ref[k, i:i + 1] = root[k:k + 1]
            high_ref[k, i:i + 1] = root[6 + k:7 + k]


def padded_rows(root_ref, low_ref, high_ref, i):
    return jnp.concatenate(
        [low_ref[0, i:i + 1], low_ref[1, i:i + 1], root_ref[i],
         high_ref[0, i:i + 1], high_ref[1, i:i + 1]], axis=0)


def weights_of(frac):
    p = 1.0 + frac
    return (
        -(p - 1.0) * (p - 2.0) * (p - 3.0) / 6.0,
        p * (p - 2.0) * (p - 3.0) / 2.0,
        -p * (p - 1.0) * (p - 3.0) / 2.0,
        p * (p - 1.0) * (p - 2.0) / 6.0,
    )


def halves(x):
    high = x.astype(BF16)
    return high, (x - high.astype(F32)).astype(BF16)


def weight_kernel(place_ref, ts_ref, tf_ref, ps_ref, pf_ref, polar_ref, both_ref, low_ref):
    diagonal = iota((32, 32), 0) == iota((32, 32), 1)

    def column(row):
        return jnp.broadcast_to(
            jnp.sum(jnp.where(diagonal, row, 0.0), axis=1, keepdims=True), (32, 128))

    start = column((ts_ref[...] - place_ref[PLACES.index("theta")] * 8 + 2).astype(F32))
    taps = weights_of(column(tf_ref[...]))
    for t in range(12):
        w = jnp.zeros((32, 128), F32)
        for k in range(4):
            w = w + jnp.where(start + k == t, taps[k], 0.0)
        polar_ref[t] = w

    lane = iota((128, NP), 0)
    side = lane % 4
    pstart = ps_ref[...] - place_ref[PLACES.index("phi")] * 32 + 2
    ptaps = weights_of(pf_ref[...])
    for n, col in enumerate((lane % 32 + 2, jnp.where(side < 2, side, side + 32))):
        w = jnp.zeros((128, NP), F32)
        for k in range(4):
            w = w + jnp.where(col == pstart + k, ptaps[k], 0.0)
        high, low = halves(w)
        both_ref[n * 128:n * 128 + 128] = high
        both_ref[n * 128 + 256:n * 128 + 384] = high
        low_ref[n * 128:n * 128 + 128] = low


def field_kernel(polar_ref, both_ref, wlow_ref, root_ref, low_ref, high_ref, out_ref, *,
                 subtrees, orders):
    def polar(i):
        rows = padded_rows(root_ref, low_ref, high_ref, i)
        total = polar_ref[0] * rows[0:1]
        for t in range(1, 12):
            total = total + polar_ref[t] * rows[t:t + 1]
        return halves(total)

    tiles, _ = places_of(orders)
    rims = [polar(16 + p) for p in range(2)]
    col = iota((32, 128), 1)
    zero = jnp.zeros((32, 128), F32)

    def masked(mask, value):
        return jnp.where(mask, value.astype(F32), zero).astype(BF16)

    for base in range(0, 16, 4):
        high, low = [], []
        for i in range(base, base + 4):
            main = polar(i)
            for j in range(4):
                _, _, rim_tile, slot = tiles[j, i]
                own = col // 32 == j
                rim = col // 4 == rim_tile % 4 * 8 + slot
                for part, out in ((0, high), (1, low)):
                    out.append(jnp.concatenate(
                        [masked(own, main[part]), masked(rim, rims[rim_tile // 4][part])], axis=1))
        high = jnp.concatenate(high, axis=0)
        low = jnp.concatenate(low, axis=0)
        field = jnp.dot(jnp.concatenate([high, low], axis=1), both_ref[...],
                        preferred_element_type=F32)
        field = field + jnp.dot(high, wlow_ref[...], preferred_element_type=F32)
        power = field * field
        for n in range(4):
            at = power[n * 128:n * 128 + 128]
            out_ref[base + n] = (
                (at[0:32] + at[32:64]) + (at[64:96] + at[96:128])) * (1.0 / subtrees)


def exchanged(blocks, axis, size):
    out = [blocks[0]]
    for k in (2, 1, 3):
        out.append(lax.ppermute(blocks[k], axis, [(i, (i + k) % size) for i in range(size)]))
    return out


def per_device(pattern, up_phi, up_theta, offsets, theta_start, theta_frac, phi_start, phi_frac):
    axes = ("c", "x", "y", AXES["z"], THETA, PHI)
    place = jnp.stack([lax.axis_index(a) for a in axes]).astype(jnp.int32)
    subs = pattern.shape[0]
    table, uphi, utheta, part = pl.pallas_call(
        prep_kernel,
        in_specs=[IN_SMEM, IN_SMEM, IN_VMEM, IN_VMEM, IN_HBM],
        out_specs=[IN_VMEM] * 4,
        out_shape=[vmem((subs, 2, NT, NP)), vmem((128, NP), BF16), vmem((NT, 64), BF16),
                   vmem((subs, 2, GROUP, 64, 128), BF16)],
        scratch_shapes=[pltpu.SemaphoreType.DMA((1,))],
        compiler_params=params(8),
        name="prep",
    )(place, *in_hbm(offsets, up_phi, up_theta.T, pattern))

    first_stage = {"x": [], "z": []}
    waiting = []
    after = []

    def first_cut():
        order, first, count, keep, other = waiting.pop(0)
        blocks = split_call(place, order, [[keep, other]])
        arrays = exchanged(blocks, AXES[order], 4)
        first_stage[order].append((first, count, arrays))
        return [blocks[0]]

    for chunk, following in zip(CHUNKS, CHUNKS[1:] + (None,)):
        order, first, count = chunk
        keep, send, part = main_call(
            chunk, following, uphi, utheta, table, part, pattern, after)
        other = lax.ppermute(send, "c", [(0, 1), (1, 0)])
        waiting.append((order, first, count, keep, other))
        after = first_cut() if len(waiting) == 2 else []
    first_cut()

    pack_in, orders = [], []
    for order, then in (("x", "z"), ("z", "x")):
        chunks = first_stage[order]
        blocks = split_call(place, then, [c[2] for c in chunks])
        pack_in += exchanged(blocks, AXES[then], 4)
        orders.append(tuple(c[:2] for c in chunks))
    orders = tuple(orders)
    blocks = pack_call(place, pack_in, orders)
    parts = exchanged(blocks, "y", 4)

    edge = vmem((2, 18, 128))
    root, low, high = pl.pallas_call(
        root_kernel,
        in_specs=[IN_VMEM] * 4,
        out_specs=[IN_VMEM] * 3,
        out_shape=[vmem((18, 8, 128)), edge, edge],
        compiler_params=params(4),
        name="root",
    )(*held(*parts))
    up = [(i, i + 1) for i in range(15)]
    below = lax.ppermute(high, THETA, up)
    above = lax.ppermute(low, THETA, [(b, a) for a, b in up])

    weights = pl.pallas_call(
        weight_kernel,
        in_specs=[IN_SMEM] + [IN_VMEM] * 4,
        out_specs=[IN_VMEM] * 3,
        out_shape=[vmem((12, 32, 128)), vmem((512, NP), BF16), vmem((256, NP), BF16)],
        compiler_params=params(4),
        name="weights",
    )(place, *in_hbm(theta_start.reshape(1, 32), theta_frac.reshape(1, 32),
                     phi_start.reshape(1, NP), phi_frac.reshape(1, NP)))
    return pl.pallas_call(
        functools.partial(field_kernel, subtrees=float(subs * 128), orders=orders),
        in_specs=[IN_VMEM] * 6,
        out_specs=IN_VMEM,
        out_shape=jax.ShapeDtypeStruct((16, 32, NP), F32),
        compiler_params=params(16),
        name="field",
    )(*held(*weights, root, below, above))


def solution(mesh):
    fine = Mesh(mesh.devices.reshape(4, 2, 4, 2, 2), ("y", "zh", "x", "zl", "c"))
    everyone = ("y", "zh", "x", "zl", "c")

    return jax.shard_map(
        per_device,
        mesh=fine,
        in_specs=(
            P(everyone, None, None, None, None), P(), P(), P(None, everyone),
            P(THETA), P(THETA), P(PHI), P(PHI),
        ),
        out_specs=P(None, THETA, PHI),
        check_vma=False,
    )
```
